8 devices in a mesh: dp: 2 (over z, y), sp: 4 (over x, core).
Axes of the slice: x: 2, y: 2, z: 1, core: 2. Of those that a mesh axis runs over, the one named last changes fastest.
Arguments:
- hidden: bfloat16 [6, 1024, 3072], P('dp', 'sp'), parts along dimension 0
- norm_w: bfloat16 [3072], replicated
- w_qkv: bfloat16 [3072, 9216], replicated
- w_out: bfloat16 [32, 96, 3072], replicated
- long_factor: float32 [48], replicated
- grad_out: bfloat16 [6, 1024, 3072], P('dp', 'sp'), parts along dimension 0
Outputs:
- output 1: bfloat16 [6, 1024, 3072], P('dp', 'sp'), parts along dimension 0
- output 2: bfloat16 [6, 1024, 3072], P('dp', 'sp'), parts along dimension 0
- output 3: float32 [6144, 9216], P('dp'), parts along dimension 0
- output 4: float32 [64, 96, 3072], P('dp'), parts along dimension 0
- output 5: float32 [6144], P('dp'), parts along dimension 0
There are 2 independent parts. The reference program is written for one: setup_inputs(seed, part) draws one part's arguments, and reference() takes and returns one part's arrays. A program takes and returns all parts, laid end to end along the dimension named above; an argument that names none is the same for every part.
All inputs are finite; a program needn't handle non-finite values.
Results may differ from the reference program's by a relative error of at most 0.011499.
Values are sent between devices in bfloat16 or wider.
A program may use at most 1 GiB of HBM per device.

```python
import math
import jax
import jax.numpy as jnp
from jax import lax

N_BATCH = 3
SEQ_LEN = 1024
D_MODEL = 3072
N_HEADS = 32
N_KV_HEADS = 32
HEAD_DIM = 96
ROT_DIM = 96

Q_WIDTH = N_HEADS * HEAD_DIM
KV_WIDTH = N_KV_HEADS * HEAD_DIM
QKV_WIDTH = Q_WIDTH + 2 * KV_WIDTH
GROUP_SIZE = N_HEADS // N_KV_HEADS
HALF_ROT = ROT_DIM // 2
NORM_EPS = 1e-5
ROPE_BASE = 10000.0
ROPE_GAIN = math.sqrt(1.0 + math.log(32.0) / math.log(4096.0))
MASK_VALUE = -1e30


def setup_inputs(seed: int = 0, part: int = 0) -> dict:
    part_key = jax.random.fold_in(jax.random.key(seed), part)
    key_hidden, key_grad = jax.random.split(part_key, 2)
    key_norm, key_qkv, key_out, key_factor = jax.random.split(jax.random.key(seed + 1), 4)
    act_shape = (N_BATCH, SEQ_LEN, D_MODEL)
    hidden = jax.random.normal(key_hidden, act_shape, jnp.float32)
    grad_out = jax.random.normal(key_grad, act_shape, jnp.float32)
    norm_w = jax.random.uniform(key_norm, (D_MODEL,), jnp.float32, 0.5, 1.5)
    w_qkv = jax.random.normal(key_qkv, (D_MODEL, QKV_WIDTH), jnp.float32) * (D_MODEL ** -0.5)
    out_std = (SEQ_LEN / (64.0 * Q_WIDTH)) ** 0.5
    w_out = jax.random.normal(key_out, (N_HEADS, HEAD_DIM, D_MODEL), jnp.float32) * out_std
    long_factor = jnp.exp(jax.random.uniform(key_factor, (HALF_ROT,), jnp.float32, 0.0, math.log(48.0)))
    return {
        'hidden': hidden.astype(jnp.bfloat16),
        'norm_w': norm_w.astype(jnp.bfloat16),
        'w_qkv': w_qkv.astype(jnp.bfloat16),
        'w_out': w_out.astype(jnp.bfloat16),
        'long_factor': long_factor,
        'grad_out': grad_out.astype(jnp.bfloat16),
    }


def to_grid(values):
    return values.astype(jnp.bfloat16).astype(jnp.float32)


def rope_tables(long_factor):
    positions = jnp.arange(SEQ_LEN).astype(jnp.float32)
    exponent = jnp.arange(HALF_ROT).astype(jnp.float32) / HALF_ROT
    inv_freq = 1.0 / (long_factor.astype(jnp.float32) * jnp.power(ROPE_BASE, exponent))
    angles = positions[:, None] * inv_freq[None, :]
    return jnp.cos(angles) * ROPE_GAIN, jnp.sin(angles) * ROPE_GAIN


def rotate(head_vals, cos_t, sin_t):
    cos_b = cos_t[None, :, None, :]
    sin_b = sin_t[None, :, None, :]
    first_half = head_vals[..., :HALF_ROT]
    second_half = head_vals[..., HALF_ROT:ROT_DIM]
    return jnp.concatenate([first_half * cos_b - second_half * sin_b, second_half * cos_b + first_half * sin_b, head_vals[..., ROT_DIM:]], axis=-1)


def head_attention(q_head, k_head, v_head):
    causal = jnp.arange(SEQ_LEN)[:, None] >= jnp.arange(SEQ_LEN)[None, :]
    scores = jnp.einsum('bqe,bse->bqs', q_head, k_head) * (HEAD_DIM ** -0.5)
    prob_mat = to_grid(jax.nn.softmax(jnp.where(causal[None], scores, MASK_VALUE), axis=-1))
    return to_grid(jnp.einsum('bqs,bse->bqe', prob_mat, v_head))


def attention(queries, key_vals, value_vals):
    head_major = jnp.moveaxis(queries, 2, 0)
    kv_index = jnp.arange(N_HEADS) // GROUP_SIZE
    saved_head = jax.checkpoint(head_attention)

    def one_head(operand):
        q_head, kv_id = operand
        k_head = lax.dynamic_index_in_dim(key_vals, kv_id, axis=2, keepdims=False)
        v_head = lax.dynamic_index_in_dim(value_vals, kv_id, axis=2, keepdims=False)
        return saved_head(q_head, k_head, v_head)

    per_head = lax.map(one_head, (head_major, kv_index))
    return jnp.moveaxis(per_head, 0, 2)


def block_forward(hidden_f, gain, w_qkv_f, w_out_f, cos_t, sin_t):
    inv_rms = lax.rsqrt(jnp.mean(hidden_f * hidden_f, axis=-1, keepdims=True) + NORM_EPS)
    normed = to_grid(hidden_f * inv_rms * gain)
    fused_qkv = jnp.dot(normed.reshape(N_BATCH * SEQ_LEN, D_MODEL), w_qkv_f, preferred_element_type=jnp.float32)
    fused_qkv = fused_qkv.reshape(N_BATCH, SEQ_LEN, QKV_WIDTH)
    queries = fused_qkv[..., :Q_WIDTH].reshape(N_BATCH, SEQ_LEN, N_HEADS, HEAD_DIM)
    key_vals = fused_qkv[..., Q_WIDTH:Q_WIDTH + KV_WIDTH].reshape(N_BATCH, SEQ_LEN, N_KV_HEADS, HEAD_DIM)
    value_vals = fused_qkv[..., Q_WIDTH + KV_WIDTH:].reshape(N_BATCH, SEQ_LEN, N_KV_HEADS, HEAD_DIM)
    attn_out = attention(to_grid(rotate(queries, cos_t, sin_t)), to_grid(rotate(key_vals, cos_t, sin_t)), to_grid(value_vals))
    projected = jnp.dot(attn_out.reshape(N_BATCH * SEQ_LEN, Q_WIDTH), w_out_f.reshape(Q_WIDTH, D_MODEL), preferred_element_type=jnp.float32)
    return (hidden_f + projected.reshape(N_BATCH, SEQ_LEN, D_MODEL)).astype(jnp.bfloat16)


def reference(hidden, norm_w, w_qkv, w_out, long_factor, grad_out):
    cos_t, sin_t = rope_tables(long_factor)

    def forward(hidden_f, gain, w_qkv_f, w_out_f):
        return block_forward(hidden_f, gain, w_qkv_f, w_out_f, cos_t, sin_t)

    block_out, pullback = jax.vjp(forward, hidden.astype(jnp.float32), norm_w.astype(jnp.float32), w_qkv.astype(jnp.float32), w_out.astype(jnp.float32))
    grad_hidden, grad_norm_w, grad_w_qkv, grad_w_out = pullback(grad_out)
    return (block_out, grad_hidden.astype(jnp.bfloat16), grad_w_qkv, grad_w_out, grad_norm_w)
```

```python
import functools
import math

import jax
import jax.numpy as jnp
from jax import lax
from jax.experimental import pallas as pl
from jax.experimental.pallas import tpu as pltpu
from jax.sharding import PartitionSpec as P


NORM_EPS = 1e-5
ROPE_BASE = 10000.0
ROPE_GAIN = math.sqrt(1.0 + math.log(32.0) / math.log(4096.0))
MASK_VALUE = -1e30
LOG2E = math.log2(math.e)
LANES = 128
CHUNK_NN, CHUNK_NT = 128, 256
VMEM_LIMIT = 60 * 1024 * 1024

ANY = pl.BlockSpec(memory_space=pl.ANY)


def params(sems):
    return pltpu.CompilerParams(dimension_semantics=sems, vmem_limit_bytes=VMEM_LIMIT)


def cost(flops, bytes_accessed, transcendentals=0):
    return pl.CostEstimate(flops=flops, bytes_accessed=bytes_accessed, transcendentals=transcendentals)


def rope_tables(seq_len, long_factor, head_dim):
    half_rot = long_factor.shape[0]
    exponent = jnp.arange(half_rot, dtype=jnp.float32) / half_rot
    inv_freq = 1.0 / (long_factor * jnp.power(ROPE_BASE, exponent))
    angles = jnp.arange(seq_len, dtype=jnp.float32)[:, None] * inv_freq[None, :]
    cos_t, sin_t = jnp.cos(angles) * ROPE_GAIN, jnp.sin(angles) * ROPE_GAIN
    pad = jnp.zeros((seq_len, LANES - head_dim), jnp.float32)
    return jnp.concatenate([cos_t, cos_t, pad], axis=1), jnp.concatenate([-sin_t, sin_t, pad], axis=1)


def lane_iota(rows):
    return lax.broadcasted_iota(jnp.int32, (rows, LANES), 1)


def swap_halves(vals, lane, half):
    return jnp.where(lane < half, pltpu.roll(vals, LANES - half, 1), pltpu.roll(vals, half, 1))


def head_of(acc, index, head_dim, lane):
    tile, off = divmod(index * head_dim, LANES)
    low = acc[:, tile * LANES:(tile + 1) * LANES]
    if off == 0:
        return low
    if off + head_dim > LANES:
        low = jnp.where(lane >= off, low, acc[:, (tile + 1) * LANES:(tile + 2) * LANES])
    return pltpu.roll(low, LANES - off, 1)


def pack_heads(heads, head_dim, lane):
    rolled = [heads[0]] + [pltpu.roll(h, LANES - (LANES - i * head_dim % LANES) % LANES, 1) for i, h in enumerate(heads) if i]
    n_tiles = len(heads) * head_dim // LANES
    return [jnp.where(lane < (t + 1) * head_dim - t * LANES, rolled[t], rolled[t + 1]) for t in range(n_tiles)]


def proj_kernel(rope, heads_blk, head_dim, me_ref, x0, x1, w, *rest):
    if rope:
        cos_ref, sin_ref, _, _, out, x_all = rest
    else:
        _, _, out, x_all = rest
    core = lax.rem(me_ref[0], 2)
    rows = CHUNK_NN if rope else CHUNK_NT
    lane = lane_iota(rows)
    col = pl.program_id(1)
    contract = (((1,), (0,)), ((), ())) if rope else (((1,), (1,)), ((), ()))

    @pl.when(col == 0)
    def _():
        x_all[0, core] = x0[0]
        x_all[0, 1 - core] = x1[0]

    ones = jnp.where(lane < head_dim, 1.0, 0.0)
    for x, place, off in [(x, place, off) for x, place in ((x0, core), (x1, 1 - core)) for off in range(0, x0.shape[1], rows)]:
        start = pl.multiple_of(place * x0.shape[1] + off, rows)
        acc = lax.dot_general(x[0, off:off + rows, :], w[...], contract, preferred_element_type=jnp.float32)
        if rope:
            plain = col >= 4
            cos_t = jnp.where(plain, ones, cos_ref[pl.ds(start, rows), :])
            sin_t = jnp.where(plain, 0.0, sin_ref[pl.ds(start, rows), :])
        for h in range(heads_blk):
            vals = head_of(acc, h, head_dim, lane)
            if rope:
                vals = vals * cos_t + swap_halves(vals, lane, head_dim // 2) * sin_t
                out[0, h, pl.ds(start, rows), :] = vals.astype(jnp.bfloat16)
            else:
                out[h, pl.ds(start, rows), :] = jnp.where(lane < head_dim, vals, 0.0).astype(jnp.bfloat16)


def project(me, x0, x1, batch0, other, w, tables, bufs, n_batch, head_dim, heads_mine):
    nb, rows, d = x0.shape
    rope = tables is not None
    heads_blk = 8
    wid = heads_blk * head_dim
    blocks = heads_mine // heads_blk
    cols = 3 * blocks if rope else blocks

    def pair(me_ref):
        own = me_ref[0] // 2
        return 1 - own if other else own

    x_spec = pl.BlockSpec((1, rows, d), lambda i, j, m: (i, 0, 0))
    if rope:
        w_spec = pl.BlockSpec((d, wid), lambda i, j, m: (0, (j // blocks) * 2 * blocks + lax.rem(m[0], 2) * blocks + lax.rem(j, blocks)))
        t_spec = pl.BlockSpec((2 * rows, LANES), lambda i, j, m: (pair(m), 0))
        o_spec = pl.BlockSpec((1, heads_blk, 2 * rows, LANES), lambda i, j, m: (j // blocks, lax.rem(j, blocks), (i + batch0) * 2 + pair(m), 0))
        o_shape = jax.ShapeDtypeStruct((3, heads_mine, n_batch * 4 * rows, LANES), jnp.bfloat16)
        extra, extra_specs = list(tables), [t_spec, t_spec]
    else:
        w_spec = pl.BlockSpec((wid, d), lambda i, j, m: (lax.rem(m[0], 2) * blocks + j, 0))
        o_spec = pl.BlockSpec((heads_blk, 2 * rows, LANES), lambda i, j, m: (j, (i + batch0) * 2 + pair(m), 0))
        o_shape = jax.ShapeDtypeStruct((heads_mine, n_batch * 4 * rows, LANES), jnp.bfloat16)
        extra, extra_specs = [], []
    a_spec = pl.BlockSpec((1, 2, rows, d), lambda i, j, m: (i + batch0, pair(m), 0, 0))
    a_shape = jax.ShapeDtypeStruct((n_batch, 4, rows, d), jnp.bfloat16)
    first = bufs is None
    if first:
        bufs = (jnp.zeros((8, LANES), jnp.bfloat16),) * 2
    n_in = 4 + len(extra)
    return pl.pallas_call(
        functools.partial(proj_kernel, rope, heads_blk, head_dim),
        grid_spec=pltpu.PrefetchScalarGridSpec(
            num_scalar_prefetch=1, grid=(nb, cols),
            in_specs=[x_spec, x_spec, w_spec] + extra_specs + [ANY, ANY],
            out_specs=[o_spec, a_spec]),
        out_shape=[o_shape, a_shape],
        input_output_aliases={} if first else {n_in: 0, n_in + 1: 1},
        compiler_params=params(("arbitrary", "arbitrary")),
        cost_estimate=cost(2 * nb * 2 * rows * d * wid * cols, nb * (cols * d * wid * 2 + 8 * rows * d)),
        name="project_qkv" if rope else "project_grad",
    )(me, x0, x1, w, *extra, *bufs)


def attn_kernel(head_dim, q, k, v, g, cos_ref, sin_ref, *rest):
    o_out, d_out, acc_o, acc_q, acc_k, acc_v = rest[-6:]
    n_heads, seq = q.shape[1], q.shape[2]
    blk = 256
    per_step = 1
    nblk = seq // blk
    scale = head_dim ** -0.5
    row = lax.broadcasted_iota(jnp.int32, (blk, blk), 0)
    column = lax.broadcasted_iota(jnp.int32, (blk, blk), 1)
    causal = row >= column
    dot = functools.partial(lax.dot_general, preferred_element_type=jnp.float32)
    nt = (((1,), (1,)), ((), ()))
    nn = (((1,), (0,)), ((), ()))
    tn = (((0,), (0,)), ((), ()))

    def some_heads(step, carry):
        for p in range(nblk):
            for h in [step * per_step + n for n in range(per_step)]:
                rows = slice(p * blk, (p + 1) * blk)
                keys = (p + 1) * blk
                qp, gp = q[0, h, rows, :], g[h, rows, :]
                kc, vc = k[0, h, :keys, :], v[0, h, :keys, :]
                s = dot(qp, kc, nt)
                diag = jnp.where(causal, s[:, p * blk:], MASK_VALUE)
                s = diag if p == 0 else jnp.concatenate([s[:, :p * blk], diag], axis=1)
                top = jnp.max(s, axis=1, keepdims=True)
                e = jnp.exp2((s - top) * (scale * LOG2E))
                prob = e * (1.0 / jnp.sum(e, axis=1, keepdims=True))
                pb = prob.astype(jnp.bfloat16)
                o = dot(pb, vc, nn)
                row_dot = jnp.sum(gp.astype(jnp.float32) * o, axis=1, keepdims=True)
                dp = dot(gp, vc, nt)
                ds = (prob * (dp - row_dot)).astype(jnp.bfloat16)
                acc_o[h, rows, :] = o
                acc_q[h, rows, :] = dot(ds, kc, nn) * scale
                dk = dot(ds, qp, tn)
                dv = dot(pb, gp, tn)
                if p:
                    acc_k[h, :p * blk, :] += dk[:p * blk]
                    acc_v[h, :p * blk, :] += dv[:p * blk]
                acc_k[h, rows, :] = dk[p * blk:]
                acc_v[h, rows, :] = dv[p * blk:]
        return carry

    lax.fori_loop(0, n_heads // per_step, some_heads, 0)

    lane = lane_iota(blk)

    def store(p, carry):
        rows = pl.ds(pl.multiple_of(p * blk, blk), blk)
        cos_t, sin_t = cos_ref[rows, :], sin_ref[rows, :]
        for which, acc in enumerate((acc_q, acc_k, acc_v, acc_o)):
            heads = []
            for h in range(n_heads):
                vals = acc[h, rows, :]
                if which == 1:
                    vals = vals * scale
                if which < 2:
                    vals = vals * cos_t - swap_halves(vals, lane, head_dim // 2) * sin_t
                heads.append(vals)
            tiles = pack_heads(heads, head_dim, lane)
            for t, vals in enumerate(tiles):
                vals = vals.astype(jnp.bfloat16)
                if which == 3:
                    o_out[0, rows, t * LANES:(t + 1) * LANES] = vals
                else:
                    d_out[which, 0, rows, t * LANES:(t + 1) * LANES] = vals
        return carry

    lax.fori_loop(0, nblk, store, 0)


def attention(qkv, grad_heads, tables, batch, bufs, n_batch, seq, head_dim):
    heads_mine = qkv.shape[1]
    group = 4
    wid = group * head_dim
    in_spec = lambda part: pl.BlockSpec((1, group, seq, LANES), lambda i, part=part: (part, i, batch, 0))
    g_spec = pl.BlockSpec((group, seq, LANES), lambda i: (i, batch, 0))
    t_spec = pl.BlockSpec((seq, LANES), lambda i: (0, 0))
    first = bufs is None
    bufs = [] if first else list(bufs)
    return pl.pallas_call(
        functools.partial(attn_kernel, head_dim),
        grid=(heads_mine // group,),
        in_specs=[in_spec(0), in_spec(1), in_spec(2), g_spec, t_spec, t_spec] + [ANY] * len(bufs),
        out_specs=[pl.BlockSpec((1, seq, wid), lambda i: (batch, 0, i)),
                   pl.BlockSpec((3, 1, seq, wid), lambda i: (0, batch, 0, i))],
        out_shape=[jax.ShapeDtypeStruct((n_batch, seq, heads_mine * head_dim), jnp.bfloat16),
                   jax.ShapeDtypeStruct((3, n_batch, seq, heads_mine * head_dim), jnp.bfloat16)],
        scratch_shapes=[pltpu.VMEM((group, seq, LANES), jnp.float32)] * 4,
        input_output_aliases={} if first else {6: 0, 7: 1},
        compiler_params=params(("arbitrary",)),
        cost_estimate=cost(heads_mine * 6 * 2 * seq * seq * 256 * 5 // 8, heads_mine * seq * 128 * 2 * 8, heads_mine * seq * seq),
        name="attention",
    )(qkv, qkv, qkv, grad_heads, *tables, *bufs)


def wgrad_kernel(me_ref, lhs, rhs, *rest):
    full, mine = rest[-2:]
    vals = lax.dot_general(lhs[...], rhs[...], (((0,), (0,)), ((), ())), preferred_element_type=jnp.float32)
    full[...] = vals
    mine[...] = vals


def weight_grad(me, lhs, rhs, full_shape, place, buf, part=None, blk_r=512, blk_c=768):
    tok, n_r = lhs.shape
    n_c = rhs.shape[-1]
    rhs_spec = pl.BlockSpec((tok, blk_c), lambda j, i, m: (0, j)) if part is None else pl.BlockSpec((None, tok, blk_c), lambda j, i, m: (part, 0, j))
    first = buf is None
    bufs = [] if first else [buf]
    return pl.pallas_call(
        wgrad_kernel,
        grid_spec=pltpu.PrefetchScalarGridSpec(
            num_scalar_prefetch=1, grid=(n_c // blk_c, n_r // blk_r),
            in_specs=[pl.BlockSpec((tok, blk_r), lambda j, i, m: (0, i)), rhs_spec] + [ANY] * len(bufs),
            out_specs=[pl.BlockSpec((blk_r, blk_c), lambda j, i, m: place(i, j, lax.rem(m[0], 2))),
                       pl.BlockSpec((blk_r, blk_c), lambda j, i, m: (i, j))]),
        out_shape=[jax.ShapeDtypeStruct(full_shape, jnp.float32), jax.ShapeDtypeStruct((n_r, n_c), jnp.float32)],
        input_output_aliases={} if first else {3: 0},
        compiler_params=params(("arbitrary", "arbitrary")),
        cost_estimate=cost(2 * tok * n_r * n_c, 2 * tok * (n_r * (n_c // blk_c) + n_c) + 8 * n_r * n_c),
        name="weight_grad",
    )(me, lhs, rhs, *bufs)


def place_kernel(me_ref, part, _, full):
    full[...] = part[...]


def place_part(me, part, full, place, blk_r=512, blk_c=1536):
    n_r, n_c = part.shape
    return pl.pallas_call(
        place_kernel,
        grid_spec=pltpu.PrefetchScalarGridSpec(
            num_scalar_prefetch=1, grid=(n_c // blk_c, n_r // blk_r),
            in_specs=[pl.BlockSpec((blk_r, blk_c), lambda j, i, m: (i, j)), ANY],
            out_specs=pl.BlockSpec((blk_r, blk_c), lambda j, i, m: place(i, j, 1 - lax.rem(m[0], 2)))),
        out_shape=jax.ShapeDtypeStruct(full.shape, jnp.float32),
        input_output_aliases={2: 0},
        compiler_params=params(("arbitrary", "arbitrary")),
        cost_estimate=cost(n_r * n_c * 40, 8 * n_r * n_c),
        name="place_part",
    )(me, part, full)


def solution(mesh):
    core_perm = [(0, 1), (1, 0), (2, 3), (3, 2)]
    chip_perm = [(0, 2), (1, 3), (2, 0), (3, 1)]
    to_core = functools.partial(lax.ppermute, axis_name='sp', perm=core_perm)
    to_chip = functools.partial(lax.ppermute, axis_name='sp', perm=chip_perm)

    def device_step(hidden, norm_w, w_qkv, w_out, long_factor, grad_out):
        n_batch, tok, d = hidden.shape
        n_heads, head_dim = w_out.shape[0], w_out.shape[1]
        heads_mine = n_heads // 2
        wid = heads_mine * head_dim
        seq = 4 * tok
        index = lax.axis_index('sp')
        me = jnp.reshape(index, (1,)).astype(jnp.int32)
        core = lax.rem(index, 2)
        partner = index + 1 - 2 * core
        w_out2 = w_out.reshape(n_heads * head_dim, d)
        tables = rope_tables(seq, long_factor, head_dim)
        gain = norm_w.astype(jnp.float32)

        hidden_f = hidden.astype(jnp.float32)
        inv_rms = lax.rsqrt(jnp.mean(hidden_f * hidden_f, axis=-1, keepdims=True) + NORM_EPS)
        normed = (hidden_f * inv_rms * gain).astype(jnp.bfloat16)

        near_n, near_g = to_core(normed), to_core(grad_out)
        far_n = [to_chip(normed[b:b + 1]) for b in range(n_batch)]
        far_g = [to_chip(grad_out[b:b + 1]) for b in range(n_batch)]

        proj = functools.partial(project, me, n_batch=n_batch, head_dim=head_dim, heads_mine=heads_mine)
        qkv = proj(normed, near_n, 0, False, w_qkv, tables, None)
        grd = proj(grad_out, near_g, 0, False, w_out2, None, None)
        relay_n = [to_core(f) for f in far_n]
        relay_g = [to_core(f) for f in far_g]
        att = None
        for b in range(n_batch):
            qkv = proj(far_n[b], relay_n[b], b, True, w_qkv, tables, qkv)
        for b in range(n_batch):
            grd = proj(far_g[b], relay_g[b], b, True, w_out2, None, grd)
            att = attention(qkv[0], grd[0], tables, b, att, n_batch, seq, head_dim)
        attn, grad_fused = att
        normed_all = qkv[1].reshape(n_batch * seq, d)
        grad_out_all = grd[1].reshape(n_batch * seq, d)

        def own_tokens(vals, axis):
            mine = lax.dynamic_slice_in_dim(vals, index * tok, tok, axis)
            theirs = lax.dynamic_slice_in_dim(vals, partner * tok, tok, axis)
            return mine, to_core(theirs)

        a_mine, a_recv = own_tokens(attn, 1)
        f_mine, f_recv = own_tokens(grad_fused, 2)

        place_o = lambda i, j, c: (c * (wid // 512) + i, j)
        g_wo, mine_wo = weight_grad(me, attn.reshape(n_batch * seq, wid), grad_out_all, (2 * wid, d), place_o, None)
        recv_wo = to_core(mine_wo)

        even = core == 0
        attn_local = jnp.concatenate([jnp.where(even, a_mine, a_recv), jnp.where(even, a_recv, a_mine)], axis=-1)
        projected = jnp.einsum('btw,wd->btd', attn_local, w_out2, preferred_element_type=jnp.float32)
        block_out = (hidden_f + projected).astype(jnp.bfloat16)

        g_wqkv, recv = None, []
        fused_tok = grad_fused.reshape(3, n_batch * seq, wid)
        for part in range(3):
            place_p = lambda i, j, c, part=part: (i, part * 4 + c * 2 + j)
            g_wqkv, mine = weight_grad(me, normed_all, fused_tok, (d, 6 * wid), place_p, g_wqkv, part)
            recv.append(to_core(mine))

        pieces = []
        for part in range(3):
            pieces += [jnp.where(even, f_mine[part], f_recv[part]), jnp.where(even, f_recv[part], f_mine[part])]
        fused_local = jnp.concatenate(pieces, axis=-1)
        grad_normed = jnp.einsum('btw,dw->btd', fused_local, w_qkv, preferred_element_type=jnp.float32)
        unit_rows = hidden_f * inv_rms
        grad_unit = grad_normed * gain
        mean_dot = jnp.mean(grad_unit * unit_rows, axis=-1, keepdims=True)
        grad_hidden = (grad_out.astype(jnp.float32) + inv_rms * (grad_unit - unit_rows * mean_dot)).astype(jnp.bfloat16)
        g_norm = jnp.sum(grad_normed * unit_rows, axis=(0, 1))
        g_norm = g_norm + to_core(g_norm)
        g_norm = g_norm + to_chip(g_norm)

        g_wo = place_part(me, recv_wo, g_wo, lambda i, j, c: (c * (wid // 512) + i, j))
        for part in range(3):
            g_wqkv = place_part(me, recv[part], g_wqkv, lambda i, j, c, part=part: (i, part * 2 + c))
        return (block_out, grad_hidden, g_wqkv, g_wo.reshape(n_heads, head_dim, d), g_norm)

    tok_spec = P('dp', 'sp', None)

    return jax.shard_map(device_step, mesh=mesh,
                         in_specs=(tok_spec, P(), P(), P(), P(), tok_spec),
                         out_specs=(tok_spec, tok_spec, P('dp', None), P('dp', None, None), P('dp')),
                         check_vma=False)
```

```python
import functools
import math

import jax
import jax.numpy as jnp
from jax import lax
from jax.experimental import pallas as pl
from jax.experimental.pallas import tpu as pltpu
from jax.sharding import PartitionSpec as P


NORM_EPS = 1e-5
ROPE_BASE = 10000.0
ROPE_GAIN = math.sqrt(1.0 + math.log(32.0) / math.log(4096.0))
MASK_VALUE = -1e30
LOG2E = math.log2(math.e)
LANES = 128
CHUNK_NN, CHUNK_NT = 128, 256
VMEM_LIMIT = 60 * 1024 * 1024

ANY = pl.BlockSpec(memory_space=pl.ANY)


def params(sems):
    return pltpu.CompilerParams(dimension_semantics=sems, vmem_limit_bytes=VMEM_LIMIT)


def cost(flops, bytes_accessed, transcendentals=0):
    return pl.CostEstimate(flops=flops, bytes_accessed=bytes_accessed, transcendentals=transcendentals)


def rope_tables(seq_len, long_factor, head_dim):
    half_rot = long_factor.shape[0]
    exponent = jnp.arange(half_rot, dtype=jnp.float32) / half_rot
    inv_freq = 1.0 / (long_factor * jnp.power(ROPE_BASE, exponent))
    angles = jnp.arange(seq_len, dtype=jnp.float32)[:, None] * inv_freq[None, :]
    cos_t, sin_t = jnp.cos(angles) * ROPE_GAIN, jnp.sin(angles) * ROPE_GAIN
    pad = jnp.zeros((seq_len, LANES - head_dim), jnp.float32)
    return jnp.concatenate([cos_t, cos_t, pad], axis=1), jnp.concatenate([-sin_t, sin_t, pad], axis=1)


def lane_iota(rows):
    return lax.broadcasted_iota(jnp.int32, (rows, LANES), 1)


def swap_halves(vals, lane, half):
    return jnp.where(lane < half, pltpu.roll(vals, LANES - half, 1), pltpu.roll(vals, half, 1))


def head_of(acc, index, head_dim, lane):
    tile, off = divmod(index * head_dim, LANES)
    low = acc[:, tile * LANES:(tile + 1) * LANES]
    if off == 0:
        return low
    if off + head_dim > LANES:
        low = jnp.where(lane >= off, low, acc[:, (tile + 1) * LANES:(tile + 2) * LANES])
    return pltpu.roll(low, LANES - off, 1)


def pack_heads(heads, head_dim, lane):
    rolled = [heads[0]] + [pltpu.roll(h, LANES - (LANES - i * head_dim % LANES) % LANES, 1) for i, h in enumerate(heads) if i]
    n_tiles = len(heads) * head_dim // LANES
    return [jnp.where(lane < (t + 1) * head_dim - t * LANES, rolled[t], rolled[t + 1]) for t in range(n_tiles)]


def proj_kernel(rope, heads_blk, head_dim, me_ref, x0, x1, w, *rest):
    if rope:
        cos_ref, sin_ref, _, _, out, x_all = rest
    else:
        _, _, out, x_all = rest
    core = lax.rem(me_ref[0], 2)
    rows = CHUNK_NN if rope else CHUNK_NT
    lane = lane_iota(rows)
    col = pl.program_id(1)
    contract = (((1,), (0,)), ((), ())) if rope else (((1,), (1,)), ((), ()))

    @pl.when(col == 0)
    def _():
        x_all[0, core] = x0[0]
        x_all[0, 1 - core] = x1[0]

    ones = jnp.where(lane < head_dim, 1.0, 0.0)
    for x, place, off in [(x, place, off) for x, place in ((x0, core), (x1, 1 - core)) for off in range(0, x0.shape[1], rows)]:
        start = pl.multiple_of(place * x0.shape[1] + off, rows)
        acc = lax.dot_general(x[0, off:off + rows, :], w[...], contract, preferred_element_type=jnp.float32)
        if rope:
            plain = col >= 4
            cos_t = jnp.where(plain, ones, cos_ref[pl.ds(start, rows), :])
            sin_t = jnp.where(plain, 0.0, sin_ref[pl.ds(start, rows), :])
        for h in range(heads_blk):
            vals = head_of(acc, h, head_dim, lane)
            if rope:
                vals = vals * cos_t + swap_halves(vals, lane, head_dim // 2) * sin_t
                out[0, h, pl.ds(start, rows), :] = vals.astype(jnp.bfloat16)
            else:
                out[h, pl.ds(start, rows), :] = jnp.where(lane < head_dim, vals, 0.0).astype(jnp.bfloat16)


def project(me, x0, x1, batch0, other, w, tables, bufs, n_batch, head_dim, heads_mine):
    nb, rows, d = x0.shape
    rope = tables is not None
    heads_blk = 8
    wid = heads_blk * head_dim
    blocks = heads_mine // heads_blk
    cols = 3 * blocks if rope else blocks

    def pair(me_ref):
        own = me_ref[0] // 2
        return 1 - own if other else own

    x_spec = pl.BlockSpec((1, rows, d), lambda i, j, m: (i, 0, 0))
    if rope:
        w_spec = pl.BlockSpec((d, wid), lambda i, j, m: (0, (j // blocks) * 2 * blocks + lax.rem(m[0], 2) * blocks + lax.rem(j, blocks)))
        t_spec = pl.BlockSpec((2 * rows, LANES), lambda i, j, m: (pair(m), 0))
        o_spec = pl.BlockSpec((1, heads_blk, 2 * rows, LANES), lambda i, j, m: (j // blocks, lax.rem(j, blocks), (i + batch0) * 2 + pair(m), 0))
        o_shape = jax.ShapeDtypeStruct((3, heads_mine, n_batch * 4 * rows, LANES), jnp.bfloat16)
        extra, extra_specs = list(tables), [t_spec, t_spec]
    else:
        w_spec = pl.BlockSpec((wid, d), lambda i, j, m: (lax.rem(m[0], 2) * blocks + j, 0))
        o_spec = pl.BlockSpec((heads_blk, 2 * rows, LANES), lambda i, j, m: (j, (i + batch0) * 2 + pair(m), 0))
        o_shape = jax.ShapeDtypeStruct((heads_mine, n_batch * 4 * rows, LANES), jnp.bfloat16)
        extra, extra_specs = [], []
    a_spec = pl.BlockSpec((1, 2, rows, d), lambda i, j, m: (i + batch0, pair(m), 0, 0))
    a_shape = jax.ShapeDtypeStruct((n_batch, 4, rows, d), jnp.bfloat16)
    first = bufs is None
    if first:
        bufs = (jnp.zeros((8, LANES), jnp.bfloat16),) * 2
    n_in = 4 + len(extra)
    return pl.pallas_call(
        functools.partial(proj_kernel, rope, heads_blk, head_dim),
        grid_spec=pltpu.PrefetchScalarGridSpec(
            num_scalar_prefetch=1, grid=(nb, cols),
            in_specs=[x_spec, x_spec, w_spec] + extra_specs + [ANY, ANY],
            out_specs=[o_spec, a_spec]),
        out_shape=[o_shape, a_shape],
        input_output_aliases={} if first else {n_in: 0, n_in + 1: 1},
        compiler_params=params(("arbitrary", "arbitrary")),
        cost_estimate=cost(2 * nb * 2 * rows * d * wid * cols, nb * (cols * d * wid * 2 + 8 * rows * d)),
        name="project_qkv" if rope else "project_grad",
    )(me, x0, x1, w, *extra, *bufs)


def attn_kernel(head_dim, q, k, v, g, cos_ref, sin_ref, *rest):
    o_out, d_out, acc_o, acc_q, acc_k, acc_v = rest[-6:]
    n_heads, seq = q.shape[1], q.shape[2]
    blk = 256
    per_step = 1
    nblk = seq // blk
    scale = head_dim ** -0.5
    row = lax.broadcasted_iota(jnp.int32, (blk, blk), 0)
    column = lax.broadcasted_iota(jnp.int32, (blk, blk), 1)
    causal = row >= column
    dot = functools.partial(lax.dot_general, preferred_element_type=jnp.float32)
    nt = (((1,), (1,)), ((), ()))
    nn = (((1,), (0,)), ((), ()))
    tn = (((0,), (0,)), ((), ()))

    def some_heads(step, carry):
        for p in range(nblk):
            for h in [step * per_step + n for n in range(per_step)]:
                rows = slice(p * blk, (p + 1) * blk)
                keys = (p + 1) * blk
                qp, gp = q[0, h, rows, :], g[h, rows, :]
                kc, vc = k[0, h, :keys, :], v[0, h, :keys, :]
                s = dot(qp, kc, nt)
                diag = jnp.where(causal, s[:, p * blk:], MASK_VALUE)
                s = diag if p == 0 else jnp.concatenate([s[:, :p * blk], diag], axis=1)
                top = jnp.max(s, axis=1, keepdims=True)
                e = jnp.exp2((s - top) * (scale * LOG2E))
                prob = e * (1.0 / jnp.sum(e, axis=1, keepdims=True))
                pb = prob.astype(jnp.bfloat16)
                o = dot(pb, vc, nn)
                row_dot = jnp.sum(gp.astype(jnp.float32) * o, axis=1, keepdims=True)
                dp = dot(gp, vc, nt)
                ds = (prob * (dp - row_dot)).astype(jnp.bfloat16)
                acc_o[h, rows, :] = o
                acc_q[h, rows, :] = dot(ds, kc, nn) * scale
                dk = dot(ds, qp, tn)
                dv = dot(pb, gp, tn)
                if p:
                    acc_k[h, :p * blk, :] += dk[:p * blk]
                    acc_v[h, :p * blk, :] += dv[:p * blk]
                acc_k[h, rows, :] = dk[p * blk:]
                acc_v[h, rows, :] = dv[p * blk:]
        return carry

    lax.fori_loop(0, n_heads // per_step, some_heads, 0)

    lane = lane_iota(blk)

    def store(p, carry):
        rows = pl.ds(pl.multiple_of(p * blk, blk), blk)
        cos_t, sin_t = cos_ref[rows, :], sin_ref[rows, :]
        for which, acc in enumerate((acc_q, acc_k, acc_v, acc_o)):
            heads = []
            for h in range(n_heads):
                vals = acc[h, rows, :]
                if which == 1:
                    vals = vals * scale
                if which < 2:
                    vals = vals * cos_t - swap_halves(vals, lane, head_dim // 2) * sin_t
                heads.append(vals)
            tiles = pack_heads(heads, head_dim, lane)
            for t, vals in enumerate(tiles):
                vals = vals.astype(jnp.bfloat16)
                if which == 3:
                    o_out[0, rows, t * LANES:(t + 1) * LANES] = vals
                else:
                    d_out[which, 0, rows, t * LANES:(t + 1) * LANES] = vals
        return carry

    lax.fori_loop(0, nblk, store, 0)


def attention(qkv, grad_heads, tables, batch, bufs, n_batch, seq, head_dim):
    heads_mine = qkv.shape[1]
    group = 4
    wid = group * head_dim
    in_spec = lambda part: pl.BlockSpec((1, group, seq, LANES), lambda i, part=part: (part, i, batch, 0))
    g_spec = pl.BlockSpec((group, seq, LANES), lambda i: (i, batch, 0))
    t_spec = pl.BlockSpec((seq, LANES), lambda i: (0, 0))
    first = bufs is None
    bufs = [] if first else list(bufs)
    return pl.pallas_call(
        functools.partial(attn_kernel, head_dim),
        grid=(heads_mine // group,),
        in_specs=[in_spec(0), in_spec(1), in_spec(2), g_spec, t_spec, t_spec] + [ANY] * len(bufs),
        out_specs=[pl.BlockSpec((1, seq, wid), lambda i: (batch, 0, i)),
                   pl.BlockSpec((3, 1, seq, wid), lambda i: (0, batch, 0, i))],
        out_shape=[jax.ShapeDtypeStruct((n_batch, seq, heads_mine * head_dim), jnp.bfloat16),
                   jax.ShapeDtypeStruct((3, n_batch, seq, heads_mine * head_dim), jnp.bfloat16)],
        scratch_shapes=[pltpu.VMEM((group, seq, LANES), jnp.float32)] * 4,
        input_output_aliases={} if first else {6: 0, 7: 1},
        compiler_params=params(("arbitrary",)),
        cost_estimate=cost(heads_mine * 6 * 2 * seq * seq * 256 * 5 // 8, heads_mine * seq * 128 * 2 * 8, heads_mine * seq * seq),
        name="attention",
    )(qkv, qkv, qkv, grad_heads, *tables, *bufs)


def wgrad_kernel(me_ref, lhs, rhs, *rest):
    full, mine = rest[-2:]
    vals = lax.dot_general(lhs[...], rhs[...], (((0,), (0,)), ((), ())), preferred_element_type=jnp.float32)
    full[...] = vals
    mine[...] = vals


def weight_grad(me, lhs, rhs, full_shape, place, buf, part=None, blk_r=256, blk_c=1536):
    tok, n_r = lhs.shape
    n_c = rhs.shape[-1]
    rhs_spec = pl.BlockSpec((tok, blk_c), lambda j, i, m: (0, j)) if part is None else pl.BlockSpec((None, tok, blk_c), lambda j, i, m: (part, 0, j))
    first = buf is None
    bufs = [] if first else [buf]
    return pl.pallas_call(
        wgrad_kernel,
        grid_spec=pltpu.PrefetchScalarGridSpec(
            num_scalar_prefetch=1, grid=(n_c // blk_c, n_r // blk_r),
            in_specs=[pl.BlockSpec((tok, blk_r), lambda j, i, m: (0, i)), rhs_spec] + [ANY] * len(bufs),
            out_specs=[pl.BlockSpec((blk_r, blk_c), lambda j, i, m: place(i, j, lax.rem(m[0], 2))),
                       pl.BlockSpec((blk_r, blk_c), lambda j, i, m: (i, j))]),
        out_shape=[jax.ShapeDtypeStruct(full_shape, jnp.float32), jax.ShapeDtypeStruct((n_r, n_c), jnp.float32)],
        input_output_aliases={} if first else {3: 0},
        compiler_params=params(("arbitrary", "arbitrary")),
        cost_estimate=cost(2 * tok * n_r * n_c, 2 * tok * (n_r * (n_c // blk_c) + n_c) + 8 * n_r * n_c),
        name="weight_grad",
    )(me, lhs, rhs, *bufs)


def dnormed_kernel(me_ref, mine, theirs, w, *rest):
    r_qkv, r_o, (out, g_qkv, g_o, sems) = rest[:3], rest[3], rest[-4:]
    step = pl.program_id(0)
    core = lax.rem(me_ref[0], 2)
    n_batch, tok, wid = mine.shape[1:]
    rows = w.shape[0]
    copies = []
    for part, ref in enumerate(r_qkv):
        at = g_qkv.at[pl.ds(step * rows, rows), pl.ds(pl.multiple_of((2 * part + 1 - core) * wid, LANES), wid)]
        copies.append(pltpu.make_async_copy(ref, at, sems.at[part]))
    rows_o = r_o.shape[0]
    copies.append(pltpu.make_async_copy(r_o, g_o.at[pl.ds((1 - core) * wid + step * rows_o, rows_o), :], sems.at[3]))
    for copy in copies:
        copy.start()
    acc = None
    for part in range(3):
        for ref, side in ((mine, core), (theirs, 1 - core)):
            cols = pl.ds(pl.multiple_of((2 * part + side) * wid, LANES), wid)
            term = lax.dot_general(ref[part].reshape(n_batch * tok, wid), w[:, cols], (((1,), (1,)), ((), ())), preferred_element_type=jnp.float32)
            acc = term if acc is None else acc + term
    out[...] = acc.reshape(out.shape)
    for copy in copies:
        copy.wait()


def grad_normed_and_place(me, fused, recv_f, w_qkv, recv, recv_o, g_qkv, g_o):
    _, n_batch, tok, wid = recv_f.shape
    d = w_qkv.shape[0]
    steps = 12
    rows, rows_o = d // steps, wid // steps
    once = pl.Buffered(buffer_count=1)
    f_spec = lambda at: pl.BlockSpec((3, n_batch, tok, wid), lambda i, m: (0, 0, at(m), 0), pipeline_mode=once)
    r_spec = pl.BlockSpec((rows, wid), lambda i, m: (i, 0))
    return pl.pallas_call(
        dnormed_kernel,
        grid_spec=pltpu.PrefetchScalarGridSpec(
            num_scalar_prefetch=1, grid=(steps,),
            in_specs=[f_spec(lambda m: m[0]), f_spec(lambda m: 0), pl.BlockSpec((rows, 6 * wid), lambda i, m: (i, 0)),
                      r_spec, r_spec, r_spec, pl.BlockSpec((rows_o, d), lambda i, m: (i, 0)), ANY, ANY],
            out_specs=[pl.BlockSpec((n_batch, tok, rows), lambda i, m: (0, 0, i)), ANY, ANY],
            scratch_shapes=[pltpu.SemaphoreType.DMA((4,))]),
        out_shape=[jax.ShapeDtypeStruct((n_batch, tok, d), jnp.float32),
                   jax.ShapeDtypeStruct(g_qkv.shape, jnp.float32), jax.ShapeDtypeStruct(g_o.shape, jnp.float32)],
        input_output_aliases={8: 1, 9: 2},
        compiler_params=params(("arbitrary",)),
        cost_estimate=cost(2 * n_batch * tok * d * 6 * wid, 12 * wid * d + 8 * d * wid * 4),
        name="grad_normed",
    )(me, fused, recv_f, w_qkv, *recv, recv_o, g_qkv, g_o)


def solution(mesh):
    core_perm = [(0, 1), (1, 0), (2, 3), (3, 2)]
    chip_perm = [(0, 2), (1, 3), (2, 0), (3, 1)]
    to_core = functools.partial(lax.ppermute, axis_name='sp', perm=core_perm)
    to_chip = functools.partial(lax.ppermute, axis_name='sp', perm=chip_perm)

    def device_step(hidden, norm_w, w_qkv, w_out, long_factor, grad_out):
        n_batch, tok, d = hidden.shape
        n_heads, head_dim = w_out.shape[0], w_out.shape[1]
        heads_mine = n_heads // 2
        wid = heads_mine * head_dim
        seq = 4 * tok
        index = lax.axis_index('sp')
        me = jnp.reshape(index, (1,)).astype(jnp.int32)
        core = lax.rem(index, 2)
        partner = index + 1 - 2 * core
        w_out2 = w_out.reshape(n_heads * head_dim, d)
        tables = rope_tables(seq, long_factor, head_dim)
        gain = norm_w.astype(jnp.float32)

        hidden_f = hidden.astype(jnp.float32)
        inv_rms = lax.rsqrt(jnp.mean(hidden_f * hidden_f, axis=-1, keepdims=True) + NORM_EPS)
        normed = (hidden_f * inv_rms * gain).astype(jnp.bfloat16)

        near_n, near_g = to_core(normed), to_core(grad_out)
        far_n = [to_chip(normed[b:b + 1]) for b in range(n_batch)]
        far_g = [to_chip(grad_out[b:b + 1]) for b in range(n_batch)]

        proj = functools.partial(project, me, n_batch=n_batch, head_dim=head_dim, heads_mine=heads_mine)
        qkv = proj(normed, near_n, 0, False, w_qkv, tables, None)
        grd = proj(grad_out, near_g, 0, False, w_out2, None, None)
        relay_n = [to_core(f) for f in far_n]
        relay_g = [to_core(f) for f in far_g]
        att = None
        for b in range(n_batch):
            qkv = proj(far_n[b], relay_n[b], b, True, w_qkv, tables, qkv)
        for b in range(n_batch):
            grd = proj(far_g[b], relay_g[b], b, True, w_out2, None, grd)
            att = attention(qkv[0], grd[0], tables, b, att, n_batch, seq, head_dim)
        attn, grad_fused = att
        normed_all = qkv[1].reshape(n_batch * seq, d)
        grad_out_all = grd[1].reshape(n_batch * seq, d)

        def own_tokens(vals, axis):
            theirs = lax.dynamic_slice_in_dim(vals, partner * tok, tok, axis)
            return to_core(theirs)

        a_mine = lax.dynamic_slice_in_dim(attn, index * tok, tok, 1)
        a_recv = own_tokens(attn, 1)
        f_recv = own_tokens(grad_fused, 2)

        place_o = lambda i, j, c: (c * (wid // 256) + i, j)
        g_wo, mine_wo = weight_grad(me, attn.reshape(n_batch * seq, wid), grad_out_all, (2 * wid, d), place_o, None)
        recv_wo = to_core(mine_wo)

        even = core == 0
        attn_local = jnp.concatenate([jnp.where(even, a_mine, a_recv), jnp.where(even, a_recv, a_mine)], axis=-1)
        projected = jnp.einsum('btw,wd->btd', attn_local, w_out2, preferred_element_type=jnp.float32)
        block_out = (hidden_f + projected).astype(jnp.bfloat16)

        g_wqkv, recv = None, []
        fused_tok = grad_fused.reshape(3, n_batch * seq, wid)
        for part in range(3):
            place_p = lambda i, j, c, part=part: (i, part * 2 + c)
            g_wqkv, mine = weight_grad(me, normed_all, fused_tok, (d, 6 * wid), place_p, g_wqkv, part)
            recv.append(to_core(mine))

        grad_normed, g_wqkv, g_wo = grad_normed_and_place(me, grad_fused, f_recv, w_qkv, recv, recv_wo, g_wqkv, g_wo)
        unit_rows = hidden_f * inv_rms
        grad_unit = grad_normed * gain
        mean_dot = jnp.mean(grad_unit * unit_rows, axis=-1, keepdims=True)
        grad_hidden = (grad_out.astype(jnp.float32) + inv_rms * (grad_unit - unit_rows * mean_dot)).astype(jnp.bfloat16)
        g_norm = jnp.sum(grad_normed * unit_rows, axis=(0, 1))
        g_norm = g_norm + to_core(g_norm)
        g_norm = g_norm + to_chip(g_norm)
        return (block_out, grad_hidden, g_wqkv, g_wo.reshape(n_heads, head_dim, d), g_norm)

    tok_spec = P('dp', 'sp', None)

    return jax.shard_map(device_step, mesh=mesh,
                         in_specs=(tok_spec, P(), P(), P(), P(), tok_spec),
                         out_specs=(tok_spec, tok_spec, P('dp', None), P('dp', None, None), P('dp')),
                         check_vma=False)
```
